32 devices in a mesh: replica: 2 (over x), tp: 16 (over z, y, core).
Axes of the slice: x: 2, y: 2, z: 4, core: 2. Of those that a mesh axis runs over, the one named last changes fastest.
Arguments:
- tokens: bfloat16 [64, 16384], P('replica', 'tp'), parts along dimension 0, may hold values from -90 to 90
- in_gain: bfloat16 [16384], replicated, may hold values from 0.5 to 1.5
- w_query: bfloat16 [16384, 8192], P(None, 'tp'), may hold values from -0.046875 to 0.046875
- w_key: bfloat16 [16384, 1024], P('tp'), may hold values from -0.09375 to 0.09375
- w_value: bfloat16 [16384, 1024], P('tp'), may hold values from -0.046875 to 0.046875
- w_out: bfloat16 [8192, 16384], P('tp'), may hold values from -0.09375 to 0.09375
- cache_keys: bfloat16 [64, 256, 1024], P('replica', 'tp'), parts along dimension 0, may hold values from -910 to 910
- cache_values: bfloat16 [64, 256, 1024], P('replica', 'tp'), parts along dimension 0, may hold values from -24 to 24
- lengths: int32 [64], P('replica'), parts along dimension 0, may hold values from 1 to 255, as said below
- post_gain: bfloat16 [16384], P('tp'), may hold values from 0.5 to 1.5
Outputs:
- hidden: bfloat16 [64, 16384], P('replica', 'tp'), parts along dimension 0
- normed: bfloat16 [64, 16384], P('replica', 'tp'), parts along dimension 0
The draws below stay inside these ranges and needn't reach their ends.
There are 2 independent parts, one for each index of `replica`. The reference program is written for one: setup_inputs(seed, part) draws one part's arguments, and reference() takes and returns one part's arrays. A program takes and returns all parts, laid end to end along the dimension named above; an argument that names none is the same for every part. Nothing has to cross between parts.
Inputs may be any that keep to these rules, and one draw needn't show every extreme that they name: `lengths`: positions already cached for each sequence; in every draw one sequence has exactly 255 and one has 8 or fewer.
All inputs are finite; a program needn't handle non-finite values.
Results may differ from the reference program's by a relative error of at most 0.019.
Values may be sent and summed in bfloat16 or wider, within the bound.
A program may use at most 128 MiB of HBM per device.

```python
import math
import jax
import jax.numpy as jnp
from jax import lax

D = 16384
HEADS = 64
KVH = 8
HD = 128
B = 32
L = 256


def draw_tokens(key, part):
    sample_key = jax.random.fold_in(jax.random.fold_in(key, 11), 0)
    sample = jnp.clip(jax.random.normal(sample_key, (B, D), jnp.float32), -6.0, 6.0)
    rising = jnp.exp(math.log(3.0) * jnp.arange(D, dtype=jnp.float32) / D)
    return (0.05 * sample * rising[None, :]).astype(jnp.bfloat16)


def head_columns(head_key):
    sample = jax.random.truncated_normal(head_key, -6.0, 6.0, (D, HD), jnp.float32)
    return sample * (1.0 / math.sqrt(D))


def projection_keys(key):
    return jax.random.split(jax.random.fold_in(key, 31), HEADS)


def draw_w_query(key, part):
    head_keys = projection_keys(key)
    columns = jax.vmap(head_columns)(head_keys)
    return jnp.transpose(columns, (1, 0, 2)).reshape(D, HEADS * HD).astype(jnp.bfloat16)


def draw_w_key(key, part):
    own_key = jax.random.fold_in(key, 41)
    sample = jax.random.truncated_normal(own_key, -6.0, 6.0, (D, KVH * HD), jnp.float32)
    return (sample * (2.0 / math.sqrt(D))).astype(jnp.bfloat16)


def draw_cache_keys(key, part):
    sample_key = jax.random.fold_in(jax.random.fold_in(key, 17), 0)
    sample = jnp.clip(jax.random.normal(sample_key, (B, L, KVH * HD), jnp.float32), -6.0, 6.0)
    return sample.astype(jnp.bfloat16)


def draw_lengths(key, part):
    drawn_key, shuffle_key, short_key = jax.random.split(jax.random.fold_in(key, 23), 3)
    lengths_drawn = jax.random.randint(drawn_key, (B,), 1, L, dtype=jnp.int32)
    shuffled = jax.random.permutation(shuffle_key, B)
    shortest = jax.random.randint(short_key, (), 1, 9, dtype=jnp.int32)
    slot_index = jnp.arange(B, dtype=jnp.int32)
    lengths_drawn = jnp.where(slot_index == shuffled[0], L - 1, lengths_drawn)
    lengths_drawn = jnp.where(slot_index == shuffled[1], shortest, lengths_drawn)
    return lengths_drawn.astype(jnp.int32)


def with_spikes(array, rng, source, target, shards_of, factor):
    def block_of(dim):
        return (jnp.arange(array.shape[dim]) // (array.shape[dim] // shards_of)).reshape((-1,) + (1,) * (array.ndim - 1 - dim))

    near = jax.random.permutation(rng, shards_of)[block_of(target)]
    far = (block_of(target) + shards_of // 2) % shards_of
    return jnp.where((block_of(source) == near) | (block_of(source) == far), factor * array, array)


def shard_levels(key, dims, cuts, low, largest):
    def one(axis_at, blocks):
        heights = jax.random.uniform(jax.random.fold_in(jax.random.fold_in(key, 6), axis_at), (blocks,), jnp.float32, low / len(cuts), largest / len(cuts))
        return jnp.repeat(jnp.exp(heights), dims[axis_at] // blocks).reshape((-1,) + (1,) * (len(dims) - axis_at - 1))

    level = one(*cuts[0])
    for cut in cuts[1:]:
        level = level * one(*cut)
    return level


def normal_values(stream_key, dims, width, most, cuts=(), kind=jnp.bfloat16):
    loudness = shard_levels(stream_key, dims, cuts, -0.22, 0.18) if cuts else 1.0
    drawn = jax.random.normal(stream_key, dims, jnp.float32) * width * loudness
    return jnp.minimum(jnp.maximum(drawn, -most), most).astype(kind)


def bell_draw_with(key, dims, deviation, limit, cuts, heavy, held_as=jnp.bfloat16):
    drawn = deviation * jax.random.normal(key, dims, jnp.float32)
    if cuts:
        drawn = drawn * shard_levels(key, dims, cuts, -0.22, 0.18)
    return jnp.clip(with_spikes(drawn, jax.random.fold_in(key, 3), *heavy), -limit, limit).astype(held_as)


def setup_inputs(seed: int = 0, part: int = 0) -> dict:
    seeds = jax.random.split(jax.random.key(seed), 11)
    part_keys = jax.random.split(jax.random.fold_in(seeds[10], part), 11)
    return {
        "tokens": draw_tokens(jax.random.fold_in(jax.random.fold_in(seeds[10], part), 71), part),
        "in_gain": jnp.clip(1.0 + 0.1 * jax.random.normal(seeds[1], (D,), jnp.float32), 0.5, 1.5).astype(jnp.bfloat16),
        "w_query": draw_w_query(jax.random.fold_in(seeds[10], 71), part),
        "w_key": draw_w_key(jax.random.fold_in(seeds[10], 71), part),
        "w_value": normal_values(seeds[4], (D, KVH * HD), D ** -0.5, 0.046875, ((0, 16),)),
        "w_out": bell_draw_with(seeds[5], (HEADS * HD, D), (HEADS * HD) ** -0.5, 0.09375, ((0, 16),), (0, 1, 16, 2.0)),
        "cache_keys": draw_cache_keys(jax.random.fold_in(jax.random.fold_in(seeds[10], part), 71), part),
        "cache_values": normal_values(part_keys[7], (B, L, KVH * HD), 4.0, 24.0, ((1, 16),)),
        "lengths": draw_lengths(jax.random.fold_in(jax.random.fold_in(seeds[10], part), 71), part),
        "post_gain": jnp.clip(1.0 + 0.1 * jax.random.normal(seeds[9], (D,), jnp.float32), 0.5, 1.5).astype(jnp.bfloat16),
    }


epsilon = 1e-05
rotary_base = 500000.0

def rotate(vectors, positions):
    half_size = vectors.shape[-1] // 2
    exponents = jnp.arange(half_size, dtype=jnp.float32) * (2.0 / vectors.shape[-1])
    frequency = jnp.power(jnp.float32(rotary_base), -exponents)
    angles = positions.astype(jnp.float32)[:, None] * frequency[None, :]
    cosine = jnp.cos(angles)[:, None, :]
    sine_part = jnp.sin(angles)[:, None, :]
    leading = vectors[..., :half_size]
    trailing = vectors[..., half_size:]
    return jnp.concatenate([leading * cosine - trailing * sine_part, trailing * cosine + leading * sine_part], axis=-1)

def inverse_rms(rows_wide):
    return lax.rsqrt(lax.optimization_barrier(jnp.mean(rows_wide * rows_wide, axis=-1, keepdims=True)) + epsilon)

def reference(tokens, in_gain, w_query, w_key, w_value, w_out, cache_keys, cache_values, lengths, post_gain):
    batch_rows = tokens.shape[0]
    capacity = cache_keys.shape[1]
    group_size = HEADS // KVH
    score_scale = 1.0 / math.sqrt(HD)
    residual = tokens.astype(jnp.float32)
    normed_in = (residual * inverse_rms(residual) * in_gain.astype(jnp.float32)).astype(jnp.bfloat16)
    query_wide = jnp.dot(normed_in, w_query, preferred_element_type=jnp.float32)
    queries = rotate(query_wide.reshape(batch_rows, HEADS, HD), lengths).astype(jnp.bfloat16)
    key_wide = jnp.dot(normed_in, w_key, preferred_element_type=jnp.float32)
    fresh_key = rotate(key_wide.reshape(batch_rows, KVH, HD), lengths).astype(jnp.bfloat16)
    fresh_value = jnp.dot(normed_in, w_value, preferred_element_type=jnp.float32).astype(jnp.bfloat16)
    fresh_value = fresh_value.reshape(batch_rows, KVH, HD)
    grouped = queries.astype(jnp.float32).reshape(batch_rows, KVH, group_size, HD)
    fresh_score = jnp.einsum('bgqd,bgd->bgq', grouped, fresh_key.astype(jnp.float32)) * score_scale
    cached_keys = cache_keys.astype(jnp.float32).reshape(batch_rows, capacity, KVH, HD)
    scores = jnp.einsum('bgqd,bpgd->bgqp', grouped, cached_keys) * score_scale
    visible = (jnp.arange(capacity, dtype=jnp.int32)[None, :] < lengths[:, None])[:, None, None, :]
    overall = jnp.maximum(lax.optimization_barrier(jnp.max(jnp.where(visible, scores, -jnp.inf), axis=-1)), fresh_score)
    weights = jnp.where(visible, jnp.exp(scores - overall[..., None]), 0.0)
    fresh_weight = jnp.exp(fresh_score - overall)
    denominator = lax.optimization_barrier(jnp.sum(weights, axis=-1)) + fresh_weight
    rounded = lax.optimization_barrier(weights.astype(jnp.bfloat16)).astype(jnp.float32)
    rounded_fresh = lax.optimization_barrier(fresh_weight.astype(jnp.bfloat16)).astype(jnp.float32)
    cached_values = cache_values.astype(jnp.float32).reshape(batch_rows, capacity, KVH, HD)
    weighted = jnp.einsum('bgqp,bpgd->bgqd', rounded, cached_values)
    weighted = weighted + rounded_fresh[..., None] * fresh_value.astype(jnp.float32)[:, :, None, :]
    head_out = (weighted / denominator[..., None]).astype(jnp.bfloat16).reshape(batch_rows, HEADS * HD)
    projected = jnp.dot(head_out, w_out, preferred_element_type=jnp.float32)
    hidden = (residual + projected).astype(jnp.bfloat16)
    hidden_wide = hidden.astype(jnp.float32)
    normed = (hidden_wide * inverse_rms(hidden_wide) * post_gain.astype(jnp.float32)).astype(jnp.bfloat16)
    return (hidden, normed)
```

```python
import functools
import math

import jax
import jax.numpy as jnp
from jax import lax
from jax.experimental import pallas as pl
from jax.experimental.pallas import tpu as pltpu
from jax.sharding import PartitionSpec as P

HEADS = 64
KVH = 8
HD = 128
GROUP = HEADS // KVH
epsilon = 1e-05
rotary_base = 500000.0
masked_value = -1e30
f32 = jnp.float32
bf16 = jnp.bfloat16


def rcopy(src, dst, send, recv, rank):
    return pltpu.make_async_remote_copy(
        src_ref=src, dst_ref=dst, send_sem=send, recv_sem=recv,
        device_id={"tp": rank}, device_id_type=pl.DeviceIdType.MESH,
    )


def merge(first, second):
    m1, l1, a1 = first
    m2, l2, a2 = second
    top = jnp.maximum(m1, m2)
    e1, e2 = jnp.exp(m1 - top), jnp.exp(m2 - top)
    return top, l1 * e1 + l2 * e2, a1 * e1 + a2 * e2


def dot(a, b, dims):
    return lax.dot_general(a, b, (dims, ((), ())), preferred_element_type=f32)


def kernel(
    n, rows, width, cols, span,
    tok, gain, wq, wk, wv, wo, ck, cv, lens, cosine, sine, pgain,
    hidden_out, normed_out,
    wq_v, wk_v, wv_v, wo_v, ck_v, cv_v, tokbuf, qbuf, acc, ssq, bias,
    kvp, kvr, kvc, kvin, kvf,
    att, ast, r1, r1s, ysend, ysends, r2, r2s, zsend, zsends, r3, r3s,
    osend, ro1, oy, ro2, oz, ro3, ss,
    s_w, s_wq, s_wo,
    tz_s, tz_r, ty_s, ty_r, tc_s, tc_r,
    qz_s, qz_r, qy_s, qy_r, qc_s, qc_r,
    kv_s, kv_r, kc_s, kc_r,
    a1_s, a1_r, a2_s, a2_r, a3_s, a3_r,
    o1_s, o1_r, o2_s, o2_r, o3_s, o3_r, ss_s, ss_r,
):
    me = lax.axis_index("tp")
    nz, half = n // 4, n // 2
    core = lax.rem(me, 2)
    chip = lax.div(me, 2)
    yy = lax.rem(chip, 2)
    zz = lax.div(chip, 2)
    heads_dev = cols // HD
    per_group = GROUP // heads_dev
    chips_per_group = max(1, per_group // 2)
    head_cols = heads_dev * rows
    scale = 1.0 / math.sqrt(HD)

    def rank_of(z, y, c):
        return z * 4 + y * 2 + c

    def zmod(k):
        return lax.rem(zz + k, nz)

    sibling = rank_of(zz, yy, 1 - core)
    across = rank_of(zz, 1 - yy, core)

    def order(index):
        k = lax.rem(index, nz)
        part = lax.div(index, nz)
        y = jnp.where(lax.rem(part, 2) == 0, yy, 1 - yy)
        c = jnp.where(part < 2, core, 1 - core)
        return rank_of(zmod(nz - k), y, c)

    def wq_copy(index):
        block = order(index)
        return pltpu.make_async_copy(
            wq.at[pl.ds(pl.multiple_of(block * width, width), width), :],
            wq_v.at[index], s_wq.at[index])

    def wo_copy(r):
        return pltpu.make_async_copy(
            wo.at[:, pl.ds(pl.multiple_of(r * width, width), width)], wo_v.at[r], s_wo.at[r])

    small = [
        pltpu.make_async_copy(a, b, s_w.at[i])
        for i, (a, b) in enumerate(((wk, wk_v), (wv, wv_v), (ck, ck_v), (cv, cv_v)))
    ]
    small[0].start()
    small[1].start()

    @pl.loop(0, n)
    def _(index):
        wq_copy(index).start()

    small[2].start()
    small[3].start()

    barrier = pltpu.get_barrier_semaphore()

    @pl.loop(1, n)
    def _(k):
        pl.semaphore_signal(
            barrier, inc=1, device_id={"tp": lax.rem(me + k, n)},
            device_id_type=pl.DeviceIdType.MESH)

    pl.semaphore_wait(barrier, n - 1)

    def gather_copies(own, buf, zs, zr, ys, yr, cs, cr):
        def z_copy(k):
            return rcopy(own, buf.at[me], zs.at[k], zr.at[k], rank_of(zmod(k), yy, core))

        def y_copy(k, src):
            block = rank_of(zmod(nz - k), yy, core)
            return rcopy(src, buf.at[block], ys.at[k], yr.at[k], across)

        def c_copy(i, block, src):
            return rcopy(src, buf.at[block], cs.at[i], cr.at[i], sibling)

        return z_copy, y_copy, c_copy

    tz, ty, tc = gather_copies(tok, tokbuf, tz_s, tz_r, ty_s, ty_r, tc_s, tc_r)

    @pl.loop(1, nz)
    def _(k):
        tz(k).start()

    ty(0, tok).start()
    tc(0, me, tok).start()

    def use_block(index, value):
        block = order(index)
        wide = value.astype(f32)
        ssq[...] += jnp.sum((wide * wide).reshape(rows, width // HD, HD), axis=1)
        scaled = (wide * gain[:, pl.ds(pl.multiple_of(block * width, width), width)]).astype(bf16)
        wq_copy(index).wait()
        acc[...] += dot(scaled, wq_v[index], ((1,), (0,)))

    acc[...] = jnp.zeros_like(acc)
    ssq[...] = jnp.zeros_like(ssq)

    own_in = (
        tok[...].astype(f32) * gain[:, pl.ds(pl.multiple_of(me * width, width), width)]
    ).astype(bf16)
    for i, w in enumerate((wk_v, wv_v)):
        small[i].wait()
        part = dot(own_in, w[...], ((1,), (0,))).astype(bf16)
        for g in range(KVH):
            kvp[i, g] = part[:, g * HD:(g + 1) * HD]
    kv_pair = rcopy(kvp.at[1 - core], kvr, kv_s.at[0], kv_r.at[0], sibling)
    kv_pair.start()
    use_block(0, tok[...])

    @pl.loop(1, nz)
    def _(k):
        tz(k).wait_recv()
        block = order(k)
        ty(k, tokbuf.at[block]).start()
        tc(k, block, tokbuf.at[block]).start()
        use_block(k, tokbuf[block])

    @pl.loop(0, nz)
    def _(k):
        block = order(nz + k)
        ty(k, tokbuf.at[block]).wait_recv()
        tc(nz + k, block, tokbuf.at[block]).start()
        use_block(nz + k, tokbuf[block])

    @pl.loop(0, n)
    def _(r):
        wo_copy(r).start()

    @pl.loop(half, n)
    def _(i):
        block = order(i)
        tc(i - half, block, tokbuf.at[block]).wait_recv()
        use_block(i, tokbuf[block])

    inverse = lax.rsqrt(jnp.sum(ssq[...], axis=1, keepdims=True) / (n * width) + epsilon)

    def rotate(v):
        return v * cosine[...] + pltpu.roll(v, HD // 2, 1) * sine[...]

    for h in range(heads_dev):
        qbuf[me, :, h * HD:(h + 1) * HD] = rotate(
            acc[:, h * HD:(h + 1) * HD] * inverse).astype(bf16)

    own_q = qbuf.at[me]
    qz, qy, qc = gather_copies(own_q, qbuf, qz_s, qz_r, qy_s, qy_r, qc_s, qc_r)

    @pl.loop(1, nz)
    def _(k):
        qz(k).start()

    qy(0, own_q).start()
    qc(0, me, own_q).start()

    keys = rows * span
    lanes = GROUP * rows
    row = lax.broadcasted_iota(jnp.int32, (keys, lanes), 0)
    column = lax.broadcasted_iota(jnp.int32, (keys, lanes), 1)
    shift = span.bit_length() - 1
    same = lax.shift_right_logical(row, shift) == (column & (rows - 1))
    seen = (me * span + (row & (span - 1))) < lens[...]
    bias[...] = jnp.where(same & seen, 0.0, masked_value)

    @pl.loop(1, nz)
    def _(k):
        qz(k).wait_recv()
        block = order(k)
        qy(k, qbuf.at[block]).start()
        qc(k, block, qbuf.at[block]).start()

    kv_pair.wait_recv()
    kvc[...] = (kvp[core].astype(f32) + kvr[...].astype(f32)).astype(bf16)

    @pl.loop(0, nz)
    def _(k):
        block = order(nz + k)
        qy(k, qbuf.at[block]).wait_recv()
        qc(nz + k, block, qbuf.at[block]).start()

    def kv_copy(k):
        other = lax.rem(chip + k, half)
        g = lax.div(other, chips_per_group)
        return rcopy(kvc.at[g], kvin.at[k], kv_s.at[k], kv_r.at[k], other * 2 + core)

    @pl.loop(1, half)
    def _(k):
        kv_copy(k).start()

    @pl.loop(half, n)
    def _(i):
        block = order(i)
        qc(i - half, block, qbuf.at[block]).wait_recv()

    small[2].wait()
    small[3].wait()

    def a1_copy(j):
        return rcopy(att.at[1 - core, j], r1.at[j], a1_s.at[j], a1_r.at[j], sibling)

    def a1s_copy(j):
        return rcopy(
            ast.at[1 - core, j], r1s.at[j], a1_s.at[half + j], a1_r.at[half + j], sibling)

    @pl.loop(0, KVH)
    def _(g):
        lane = pl.ds(pl.multiple_of(g * HD, HD), HD)
        k_g = ck_v[:, :, lane].reshape(keys, HD)
        v_g = cv_v[:, :, lane].reshape(keys, HD)
        q_g = jnp.concatenate([
            qbuf[g * per_group + i // heads_dev, :,
                 (i % heads_dev) * HD:(i % heads_dev + 1) * HD]
            for i in range(GROUP)], axis=0)
        s = dot(k_g, q_g, ((1,), (1,))) * scale + bias[...]
        top = jnp.max(s, axis=0, keepdims=True)
        p = jnp.exp(s - top)
        total = jnp.sum(p, axis=0, keepdims=True)
        a = dot(v_g, p.astype(bf16), ((0,), (0,))).astype(bf16)
        for t in range(per_group):
            j = g * (per_group // 2) + t // 2
            att[t % 2, j] = a[:, t * head_cols:(t + 1) * head_cols]
            ast[t % 2, j, 0:1] = top[:, t * head_cols:(t + 1) * head_cols]
            ast[t % 2, j, 1:2] = total[:, t * head_cols:(t + 1) * head_cols]
        for t in range(per_group // 2):
            a1_copy(g * (per_group // 2) + t).start()
            a1s_copy(g * (per_group // 2) + t).start()

    def triple(values, stats):
        return stats[0:1], stats[1:2], values.astype(f32)

    def chip_part(j):
        a1_copy(j).wait_recv()
        a1s_copy(j).wait_recv()
        return merge(triple(att[core, j], ast[core, j]), triple(r1[j], r1s[j]))

    def a2_copy(z):
        return rcopy(ysend.at[z], r2.at[z], a2_s.at[z], a2_r.at[z], across)

    def a2s_copy(z):
        return rcopy(ysends.at[z], r2s.at[z], a2_s.at[nz + z], a2_r.at[nz + z], across)

    def a3_copy(k):
        return rcopy(zsend.at[k], r3.at[k], a3_s.at[k], a3_r.at[k], rank_of(zmod(k), yy, core))

    def a3s_copy(k):
        return rcopy(
            zsends.at[k], r3s.at[k], a3_s.at[nz + k], a3_r.at[nz + k],
            rank_of(zmod(k), yy, core))

    @pl.loop(0, nz)
    def _(k):
        z = zmod(k + 1)
        m, l, a = chip_part(z * 2 + 1 - yy)
        ysend[z] = a.astype(bf16)
        ysends[z, 0:1] = m
        ysends[z, 1:2] = l
        a2_copy(z).start()
        a2s_copy(z).start()

    def pair_part(z):
        mine = chip_part(z * 2 + yy)
        a2_copy(z).wait_recv()
        a2s_copy(z).wait_recv()
        return merge(mine, triple(r2[z], r2s[z]))

    @pl.loop(1, nz)
    def _(k):
        m, l, a = pair_part(zmod(k))
        zsend[k] = a.astype(bf16)
        zsends[k, 0:1] = m
        zsends[k, 1:2] = l
        a3_copy(k).start()
        a3s_copy(k).start()

    own = pair_part(zz)

    my_group = lax.div(chip, chips_per_group)
    fresh = kvc[my_group].astype(f32)
    for k in range(1, half):
        kv_copy(k).wait_recv()
        fresh = fresh + kvin[k].astype(f32)
    kvf[core] = fresh
    kv_out = rcopy(kvf.at[core], kvf.at[core], kc_s.at[0], kc_r.at[0], sibling)
    kv_out.start()
    rcopy(kvf.at[1 - core], kvf.at[1 - core], kc_s.at[0], kc_r.at[0], sibling).wait_recv()
    fresh_key = rotate(kvf[0] * inverse).astype(bf16)
    fresh_value = (kvf[1] * inverse).astype(bf16)
    q_own = jnp.concatenate(
        [qbuf[me, :, h * HD:(h + 1) * HD] for h in range(heads_dev)], axis=0)
    sf = dot(fresh_key, q_own, ((1,), (1,))) * scale
    frow = lax.broadcasted_iota(jnp.int32, (rows, head_cols), 0)
    fcol = lax.broadcasted_iota(jnp.int32, (rows, head_cols), 1)
    sf = jnp.where(frow == (fcol & (rows - 1)), sf, masked_value)
    top_f = jnp.max(sf, axis=0, keepdims=True)
    pf = jnp.exp(sf - top_f)
    own = merge(own, (
        top_f, jnp.sum(pf, axis=0, keepdims=True),
        dot(fresh_value, pf.astype(bf16), ((0,), (0,)))))
    for k in range(1, nz):
        a3_copy(k).wait_recv()
        a3s_copy(k).wait_recv()
        own = merge(own, triple(r3[k], r3s[k]))
    head_t = jnp.transpose(own[2] / own[1])
    head_rows = jnp.concatenate(
        [head_t[h * rows:(h + 1) * rows] for h in range(heads_dev)], axis=1).astype(bf16)

    @pl.loop(0, n)
    def _(r):
        wo_copy(r).wait()

    def project(r):
        return dot(head_rows, wo_v[r], ((1,), (0,)))

    def o1_copy(i):
        return rcopy(osend.at[i], ro1.at[i], o1_s.at[i], o1_r.at[i], sibling)

    def o2_copy(k):
        return rcopy(oy.at[k], ro2.at[k], o2_s.at[k], o2_r.at[k], across)

    def o3_copy(k):
        return rcopy(oz.at[k], ro3.at[k], o3_s.at[k], o3_r.at[k], rank_of(zmod(k), yy, core))

    def target(i, y_first):
        k = lax.rem(i + 1, nz)
        y = jnp.where(i < nz, y_first, 1 - y_first)
        return zmod(k), y

    @pl.loop(0, half)
    def _(i):
        z, y = target(i, 1 - yy)
        osend[i] = project(rank_of(z, y, 1 - core)).astype(bf16)
        o1_copy(i).start()

    @pl.loop(0, nz)
    def _(i):
        z, y = target(i, 1 - yy)
        value = project(rank_of(z, y, core))
        o1_copy(i).wait_recv()
        oy[i] = (value + ro1[i].astype(f32)).astype(bf16)
        o2_copy(i).start()

    def out_part(i):
        z, y = target(nz + i, 1 - yy)
        value = project(rank_of(z, y, core))
        o1_copy(nz + i).wait_recv()
        value = value + ro1[nz + i].astype(f32)
        o2_copy(i).wait_recv()
        return value + ro2[i].astype(f32)

    @pl.loop(0, nz - 1)
    def _(i):
        oz[i + 1] = out_part(i).astype(bf16)
        o3_copy(i + 1).start()

    summed = out_part(nz - 1)
    for k in range(1, nz):
        o3_copy(k).wait_recv()
        summed = summed + ro3[k].astype(f32)
    hidden = (tok[...].astype(f32) + summed).astype(bf16)
    hidden_out[...] = hidden
    wide = hidden.astype(f32)
    square = jnp.sum(wide * wide, axis=1, keepdims=True)
    diagonal = (
        lax.broadcasted_iota(jnp.int32, (rows, HD), 0)
        == lax.broadcasted_iota(jnp.int32, (rows, HD), 1))
    ss[0] = jnp.sum(jnp.where(diagonal, square, 0.0), axis=0, keepdims=True)

    def ss_copy(k):
        return rcopy(ss.at[0], ss.at[k], ss_s.at[k], ss_r.at[k], lax.rem(me + k, n))

    @pl.loop(1, n)
    def _(k):
        ss_copy(k).start()

    total = ss[0]
    for k in range(1, n):
        ss_copy(k).wait_recv()
        total = total + ss[k]
    mean = jnp.sum(jnp.where(diagonal, total, 0.0), axis=1, keepdims=True) / (n * width)
    normed_out[...] = (wide * lax.rsqrt(mean + epsilon) * pgain[...]).astype(bf16)

    @pl.loop(1, nz)
    def _(k):
        tz(k).wait_send()
        qz(k).wait_send()
        a3_copy(k).wait_send()
        a3s_copy(k).wait_send()
        o3_copy(k).wait_send()

    @pl.loop(0, nz)
    def _(k):
        ty(k, tok).wait_send()
        qy(k, own_q).wait_send()
        a2_copy(k).wait_send()
        a2s_copy(k).wait_send()
        o2_copy(k).wait_send()

    @pl.loop(0, half)
    def _(k):
        tc(k, me, tok).wait_send()
        qc(k, me, own_q).wait_send()
        a1_copy(k).wait_send()
        a1s_copy(k).wait_send()
        o1_copy(k).wait_send()

    @pl.loop(1, half)
    def _(k):
        kv_copy(k).wait_send()

    @pl.loop(1, n)
    def _(k):
        ss_copy(k).wait_send()

    kv_pair.wait_send()
    kv_out.wait_send()


def local(n, tokens, in_gain, w_query, w_key, w_value, w_out, cache_keys, cache_values, lengths,
          post_gain):
    rows, width = tokens.shape
    cols = w_query.shape[1]
    span = cache_keys.shape[1]
    kv_width = w_key.shape[1]
    heads_dev = cols // HD
    head_cols = heads_dev * rows
    nz, half = n // 4, n // 2
    exponents = jnp.arange(HD // 2, dtype=f32) * (2.0 / HD)
    frequency = jnp.power(f32(rotary_base), -exponents)
    angles = lengths.astype(f32)[:, None] * frequency[None, :]
    cosine, sine = jnp.cos(angles), jnp.sin(angles)
    cosine = jnp.concatenate([cosine, cosine], axis=1)
    sine = jnp.concatenate([-sine, sine], axis=1)
    lens = jnp.tile(lengths, GROUP)[None, :]
    vm = pl.BlockSpec(memory_space=pltpu.VMEM)
    hbm = pl.BlockSpec(memory_space=pl.ANY)
    V = pltpu.VMEM
    dma = lambda k: pltpu.SemaphoreType.DMA((k,))
    attn = lambda k: V((k, HD, head_cols), bf16)
    stat = lambda k: V((k, 2, head_cols), f32)
    block = lambda k: V((k, rows, width), bf16)
    scratch = [
        V((n, width, cols), bf16), V((width, kv_width), bf16), V((width, kv_width), bf16),
        V((n, cols, width), bf16), V(cache_keys.shape, bf16), V(cache_values.shape, bf16),
        block(n), V((n, rows, cols), bf16), V((rows, cols), f32), V((rows, HD), f32),
        V((rows * span, GROUP * rows), f32),
        V((2, KVH, rows, HD), bf16), V((KVH, rows, HD), bf16), V((KVH, rows, HD), bf16),
        V((half, rows, HD), bf16), V((2, rows, HD), f32),
        V((2, half, HD, head_cols), bf16), V((2, half, 2, head_cols), f32),
        attn(half), stat(half), attn(nz), stat(nz), attn(nz), stat(nz), attn(nz), stat(nz),
        attn(nz), stat(nz),
        block(half), block(half), block(nz), block(nz), block(nz), block(nz),
        V((n, 1, HD), f32),
        dma(4), dma(n), dma(n),
        dma(nz), dma(nz), dma(nz), dma(nz), dma(half), dma(half),
        dma(nz), dma(nz), dma(nz), dma(nz), dma(half), dma(half),
        dma(half), dma(half), dma(1), dma(1),
        dma(n), dma(n), dma(half), dma(half), dma(half), dma(half),
        dma(half), dma(half), dma(nz), dma(nz), dma(nz), dma(nz), dma(n), dma(n),
    ]
    return pl.pallas_call(
        functools.partial(kernel, n, rows, width, cols, span),
        out_shape=(jax.ShapeDtypeStruct((rows, width), bf16),) * 2,
        in_specs=[vm, vm, hbm, hbm, hbm, hbm, hbm, hbm, vm, vm, vm, vm],
        out_specs=(vm, vm),
        scratch_shapes=scratch,
        compiler_params=pltpu.CompilerParams(
            collective_id=0, has_side_effects=True, vmem_limit_bytes=67043328),
    )(
        tokens, in_gain.astype(f32)[None, :], w_query, w_key, w_value, w_out, cache_keys,
        cache_values, lens, cosine, sine, post_gain.astype(f32)[None, :],
    )


def solution(mesh):
    placed = (
        P("replica", "tp"),
        P(),
        P(None, "tp"),
        P("tp", None),
        P("tp", None),
        P("tp", None),
        P("replica", "tp", None),
        P("replica", "tp", None),
        P("replica"),
        P("tp"),
    )
    return jax.shard_map(
        functools.partial(local, mesh.shape["tp"]),
        mesh=mesh,
        in_specs=placed,
        out_specs=(P("replica", "tp"), P("replica", "tp")),
        check_vma=False,
    )
```

```python
import functools
import math

import jax
import jax.numpy as jnp
from jax import lax
from jax.experimental import pallas as pl
from jax.experimental.pallas import tpu as pltpu
from jax.sharding import PartitionSpec as P

HEADS = 64
KVH = 8
HD = 128
GROUP = HEADS // KVH
epsilon = 1e-05
rotary_base = 500000.0
masked_value = -1e30
f32 = jnp.float32
bf16 = jnp.bfloat16


def rcopy(src, dst, send, recv, rank):
    return pltpu.make_async_remote_copy(
        src_ref=src, dst_ref=dst, send_sem=send, recv_sem=recv,
        device_id={"tp": rank}, device_id_type=pl.DeviceIdType.MESH,
    )


def merge(first, second):
    m1, l1, a1 = first
    m2, l2, a2 = second
    top = jnp.maximum(m1, m2)
    e1, e2 = jnp.exp(m1 - top), jnp.exp(m2 - top)
    return top, l1 * e1 + l2 * e2, a1 * e1 + a2 * e2


def dot(a, b, dims):
    return lax.dot_general(a, b, (dims, ((), ())), preferred_element_type=f32)


def kernel(
    n, rows, width, cols, span,
    tok, gain_in, post_in, lens_in, wq, wk, wv, wo, ck, cv,
    out,
    gain, cosine, sine, hid_v, nrm_v, s_out,
    wq_v, wk_v, wv_v, wo_v, ck_v, cv_v, tokbuf, qbuf, acc, ssq, bias,
    kvp, kvr, kvc, kvin, kvf,
    att, ast, r1, r1s, ysend, ysends, r2, r2s, zsend, zsends, r3, r3s,
    osend, ro1, oy, ro2, oz, ro3, ss,
    s_w, s_wq, s_wo,
    tz_s, tz_r, ty_s, ty_r, tc_s, tc_r,
    qz_s, qz_r, qy_s, qy_r, qc_s, qc_r,
    kv_s, kv_r, kc_s, kc_r,
    a1_s, a1_r, a2_s, a2_r, a3_s, a3_r,
    o1_s, o1_r, o2_s, o2_r, o3_s, o3_r, ss_s, ss_r,
):
    me = lax.axis_index("tp")
    nz, half = n // 4, n // 2
    core = lax.rem(me, 2)
    chip = lax.div(me, 2)
    yy = lax.rem(chip, 2)
    zz = lax.div(chip, 2)
    heads_dev = cols // HD
    per_group = GROUP // heads_dev
    chips_per_group = max(1, per_group // 2)
    head_cols = heads_dev * rows
    scale = 1.0 / math.sqrt(HD)

    def rank_of(z, y, c):
        return z * 4 + y * 2 + c

    def zmod(k):
        return lax.rem(zz + k, nz)

    def off(i):
        return lax.rem(jnp.where(zz >= nz // 2, i, nz - i), nz)

    sibling = rank_of(zz, yy, 1 - core)
    across = rank_of(zz, 1 - yy, core)

    def order(index):
        k = lax.rem(index, nz)
        part = lax.div(index, nz)
        y = jnp.where(lax.rem(part, 2) == 0, yy, 1 - yy)
        c = jnp.where(part < 2, core, 1 - core)
        return rank_of(zmod(nz - off(k)), y, c)

    def wq_copy(index):
        block = order(index)
        return pltpu.make_async_copy(
            wq.at[pl.ds(pl.multiple_of(block * width, width), width), :],
            wq_v.at[index], s_wq.at[index])

    def wo_copy(r):
        return pltpu.make_async_copy(
            wo.at[:, pl.ds(pl.multiple_of(r * width, width), width)], wo_v.at[r], s_wo.at[r])

    small = [
        pltpu.make_async_copy(a, b, s_w.at[i])
        for i, (a, b) in enumerate(((wk, wk_v), (wv, wv_v), (ck, ck_v), (cv, cv_v)))
    ]
    @pl.loop(0, half)
    def _(index):
        wq_copy(index).start()
        wq_copy(half + index).start()

    for copy in small:
        copy.start()

    barrier = pltpu.get_barrier_semaphore()

    @pl.loop(1, n)
    def _(k):
        pl.semaphore_signal(
            barrier, inc=1, device_id={"tp": lax.rem(me + k, n)},
            device_id_type=pl.DeviceIdType.MESH)

    wide_gain = gain_in[...].astype(f32)
    for i in range(n * width // HD):
        gain[:, i * HD:(i + 1) * HD] = wide_gain[i:i + 1]
    sub = lax.broadcasted_iota(jnp.int32, (rows, rows), 0)
    lane_b = lax.broadcasted_iota(jnp.int32, (rows, rows), 1)
    len_column = jnp.sum(
        jnp.where(sub == lane_b, lens_in[...].astype(f32), 0.0), axis=1, keepdims=True)
    lanes = GROUP * rows
    sub = lax.broadcasted_iota(jnp.int32, (rows, lanes), 0)
    lane_b = lax.broadcasted_iota(jnp.int32, (rows, lanes), 1) & (rows - 1)
    lens = jnp.sum(jnp.where(sub == lane_b, len_column, 0.0), axis=0, keepdims=True)
    lane = lax.broadcasted_iota(jnp.int32, (rows, HD), 1)
    exponent = (lane & (HD // 2 - 1)).astype(f32) * (2.0 / HD)
    angle = len_column * jnp.exp(exponent * (-math.log(rotary_base)))
    cosine[...] = jnp.cos(angle)
    sine[...] = jnp.where(lane < HD // 2, -1.0, 1.0) * jnp.sin(angle)
    acc[...] = jnp.zeros_like(acc)
    ssq[...] = jnp.zeros_like(ssq)

    pl.semaphore_wait(barrier, n - 1)

    def gather_copies(own, buf, zs, zr, ys, yr, cs, cr):
        def z_copy(k):
            return rcopy(own, buf.at[me], zs.at[k], zr.at[k], rank_of(zmod(k), yy, core))

        def y_copy(k, src):
            block = rank_of(zmod(nz - off(k)), yy, core)
            return rcopy(src, buf.at[block], ys.at[k], yr.at[k], across)

        def c_copy(i, block, src):
            return rcopy(src, buf.at[block], cs.at[i], cr.at[i], sibling)

        return z_copy, y_copy, c_copy

    tz, ty, tc = gather_copies(tok, tokbuf, tz_s, tz_r, ty_s, ty_r, tc_s, tc_r)

    @pl.loop(1, nz)
    def _(k):
        tz(off(k)).start()

    ty(0, tok).start()
    tc(0, me, tok).start()

    def use_block(index, value):
        block = order(index)
        wide = value.astype(f32)
        ssq[...] += jnp.sum((wide * wide).reshape(rows, width // HD, HD), axis=1)
        scaled = (wide * gain[:, pl.ds(pl.multiple_of(block * width, width), width)]).astype(bf16)
        wq_copy(index).wait()
        acc[...] += dot(scaled, wq_v[index], ((1,), (0,)))

    use_block(0, tok[...])

    def use_sibling(i):
        block = order(half + i)
        tc(i, block, tokbuf.at[block]).wait_recv()
        use_block(half + i, tokbuf[block])

    @pl.loop(1, nz)
    def _(k):
        tz(off(k)).wait_recv()
        block = order(k)
        ty(k, tokbuf.at[block]).start()
        tc(k, block, tokbuf.at[block]).start()
        use_block(k, tokbuf[block])
        use_sibling(k - 1)

    @pl.loop(0, nz)
    def _(k):
        block = order(nz + k)
        ty(k, tokbuf.at[block]).wait_recv()
        tc(nz + k, block, tokbuf.at[block]).start()
        use_block(nz + k, tokbuf[block])
        use_sibling(nz + k - 1)

    @pl.loop(0, n)
    def _(r):
        wo_copy(r).start()

    use_sibling(half - 1)

    inverse = lax.rsqrt(jnp.sum(ssq[...], axis=1, keepdims=True) / (n * width) + epsilon)

    def rotate(v):
        return v * cosine[...] + pltpu.roll(v, HD // 2, 1) * sine[...]

    for h in range(heads_dev):
        qbuf[me, :, h * HD:(h + 1) * HD] = rotate(
            acc[:, h * HD:(h + 1) * HD] * inverse).astype(bf16)

    own_q = qbuf.at[me]
    qz, qy, qc = gather_copies(own_q, qbuf, qz_s, qz_r, qy_s, qy_r, qc_s, qc_r)

    @pl.loop(1, nz)
    def _(k):
        qz(off(k)).start()

    qy(0, own_q).start()
    qc(0, me, own_q).start()

    own_in = (
        tok[...].astype(f32) * gain[:, pl.ds(pl.multiple_of(me * width, width), width)]
    ).astype(bf16)
    for i, w in enumerate((wk_v, wv_v)):
        small[i].wait()
        part = dot(own_in, w[...], ((1,), (0,))).astype(bf16)
        for g in range(KVH):
            kvp[i, g] = part[:, g * HD:(g + 1) * HD]
    kv_pair = rcopy(kvp.at[1 - core], kvr, kv_s.at[0], kv_r.at[0], sibling)
    kv_pair.start()

    keys = rows * span
    row = lax.broadcasted_iota(jnp.int32, (keys, lanes), 0)
    column = lax.broadcasted_iota(jnp.int32, (keys, lanes), 1)
    shift = span.bit_length() - 1
    same = lax.shift_right_logical(row, shift) == (column & (rows - 1))
    seen = (me * span + (row & (span - 1))).astype(f32) < lens
    bias[...] = jnp.where(same & seen, 0.0, masked_value)

    @pl.loop(1, nz)
    def _(k):
        qz(off(k)).wait_recv()
        block = order(k)
        qy(k, qbuf.at[block]).start()
        qc(k, block, qbuf.at[block]).start()

    kv_pair.wait_recv()
    kvc[...] = (kvp[core].astype(f32) + kvr[...].astype(f32)).astype(bf16)

    @pl.loop(0, nz)
    def _(k):
        block = order(nz + k)
        qy(k, qbuf.at[block]).wait_recv()
        qc(nz + k, block, qbuf.at[block]).start()

    def kv_copy(k):
        other = lax.rem(chip + k, half)
        g = lax.div(other, chips_per_group)
        return rcopy(kvc.at[g], kvin.at[k], kv_s.at[k], kv_r.at[k], other * 2 + core)

    @pl.loop(1, half)
    def _(k):
        kv_copy(k).start()

    @pl.loop(half, n)
    def _(i):
        block = order(i)
        qc(i - half, block, qbuf.at[block]).wait_recv()

    small[2].wait()
    small[3].wait()

    def a1_copy(j):
        return rcopy(att.at[1 - core, j], r1.at[j], a1_s.at[j], a1_r.at[j], sibling)

    def a1s_copy(j):
        return rcopy(
            ast.at[1 - core, j], r1s.at[j], a1_s.at[half + j], a1_r.at[half + j], sibling)

    def attend(g):
        lane = pl.ds(pl.multiple_of(g * HD, HD), HD)
        k_g = ck_v[:, :, lane].reshape(keys, HD)
        v_g = cv_v[:, :, lane].reshape(keys, HD)
        q_g = jnp.concatenate([
            qbuf[g * per_group + i // heads_dev, :,
                 (i % heads_dev) * HD:(i % heads_dev + 1) * HD]
            for i in range(GROUP)], axis=0)
        s = dot(k_g, q_g, ((1,), (1,))) * scale + bias[...]
        top = jnp.max(s, axis=0, keepdims=True)
        p = jnp.exp(s - top)
        total = jnp.sum(p, axis=0, keepdims=True)
        a = dot(v_g, p.astype(bf16), ((0,), (0,))).astype(bf16)
        for t in range(per_group):
            j = g * (per_group // 2) + t // 2
            att[t % 2, j] = a[:, t * head_cols:(t + 1) * head_cols]
            ast[t % 2, j, 0:1] = top[:, t * head_cols:(t + 1) * head_cols]
            ast[t % 2, j, 1:2] = total[:, t * head_cols:(t + 1) * head_cols]
        for t in range(per_group // 2):
            a1_copy(g * (per_group // 2) + t).start()
            a1s_copy(g * (per_group // 2) + t).start()

    def triple(values, stats):
        return stats[0:1], stats[1:2], values.astype(f32)

    def chip_part(j):
        a1_copy(j).wait_recv()
        a1s_copy(j).wait_recv()
        return merge(triple(att[core, j], ast[core, j]), triple(r1[j], r1s[j]))

    def a2_copy(z):
        return rcopy(ysend.at[z], r2.at[z], a2_s.at[z], a2_r.at[z], across)

    def a2s_copy(z):
        return rcopy(ysends.at[z], r2s.at[z], a2_s.at[nz + z], a2_r.at[nz + z], across)

    def a3_copy(k):
        return rcopy(zsend.at[k], r3.at[k], a3_s.at[k], a3_r.at[k], rank_of(zmod(k), yy, core))

    def a3s_copy(k):
        return rcopy(
            zsends.at[k], r3s.at[k], a3_s.at[nz + k], a3_r.at[nz + k],
            rank_of(zmod(k), yy, core))

    kv_out = rcopy(kvf.at[core], kvf.at[core], kc_s.at[0], kc_r.at[0], sibling)

    def sum_fresh():
        my_group = lax.div(chip, chips_per_group)
        fresh = kvc[my_group].astype(f32)
        for k in range(1, half):
            kv_copy(k).wait_recv()
            fresh = fresh + kvin[k].astype(f32)
        kvf[core] = fresh
        kv_out.start()

    def y_stage(k):
        z = zmod(off(lax.rem(k + 1, nz)))
        m, l, a = chip_part(z * 2 + 1 - yy)
        ysend[z] = a.astype(bf16)
        ysends[z, 0:1] = m
        ysends[z, 1:2] = l
        a2_copy(z).start()
        a2s_copy(z).start()

    def pair_part(z):
        mine = chip_part(z * 2 + yy)
        a2_copy(z).wait_recv()
        a2s_copy(z).wait_recv()
        return merge(mine, triple(r2[z], r2s[z]))

    def z_stage(i):
        k = off(i)
        m, l, a = pair_part(zmod(k))
        zsend[k] = a.astype(bf16)
        zsends[k, 0:1] = m
        zsends[k, 1:2] = l
        a3_copy(k).start()
        a3s_copy(k).start()

    if half == KVH:
        def send_order(i):
            y = jnp.where(i < nz, 1 - yy, yy)
            return zmod(off(lax.rem(i + 1, nz))) * 2 + y

        attend(send_order(0))
        attend(send_order(1))

        @pl.loop(0, nz)
        def _(k):
            attend(send_order(k + 2))
            y_stage(k)

        sum_fresh()

        @pl.loop(1, nz - 1)
        def _(k):
            attend(send_order(nz + k + 1))
            z_stage(k)

        z_stage(nz - 1)
    else:
        pl.loop(0, KVH)(attend)
        pl.loop(0, nz)(y_stage)
        sum_fresh()
        pl.loop(1, nz)(z_stage)

    own = pair_part(zz)

    rcopy(kvf.at[1 - core], kvf.at[1 - core], kc_s.at[0], kc_r.at[0], sibling).wait_recv()
    fresh_key = rotate(kvf[0] * inverse).astype(bf16)
    fresh_value = (kvf[1] * inverse).astype(bf16)
    q_own = jnp.concatenate(
        [qbuf[me, :, h * HD:(h + 1) * HD] for h in range(heads_dev)], axis=0)
    sf = dot(fresh_key, q_own, ((1,), (1,))) * scale
    frow = lax.broadcasted_iota(jnp.int32, (rows, head_cols), 0)
    fcol = lax.broadcasted_iota(jnp.int32, (rows, head_cols), 1)
    sf = jnp.where(frow == (fcol & (rows - 1)), sf, masked_value)
    top_f = jnp.max(sf, axis=0, keepdims=True)
    pf = jnp.exp(sf - top_f)
    own = merge(own, (
        top_f, jnp.sum(pf, axis=0, keepdims=True),
        dot(fresh_value, pf.astype(bf16), ((0,), (0,)))))
    for k in range(1, nz):
        a3_copy(k).wait_recv()
        a3s_copy(k).wait_recv()
        own = merge(own, triple(r3[k], r3s[k]))
    head_t = jnp.transpose(own[2] / own[1])
    head_rows = jnp.concatenate(
        [head_t[h * rows:(h + 1) * rows] for h in range(heads_dev)], axis=1).astype(bf16)

    @pl.loop(0, n)
    def _(r):
        wo_copy(r).wait()

    def project(r):
        return dot(head_rows, wo_v[r], ((1,), (0,)))

    def o1_copy(i):
        return rcopy(osend.at[i], ro1.at[i], o1_s.at[i], o1_r.at[i], sibling)

    def o2_copy(k):
        return rcopy(oy.at[k], ro2.at[k], o2_s.at[k], o2_r.at[k], across)

    def o3_copy(k):
        return rcopy(oz.at[k], ro3.at[k], o3_s.at[k], o3_r.at[k], rank_of(zmod(k), yy, core))

    def target(i, y_first):
        k = off(lax.rem(i + 1, nz))
        y = jnp.where(i < nz, y_first, 1 - y_first)
        return zmod(k), y

    def for_sibling(i):
        z, y = target(i, 1 - yy)
        osend[i] = project(rank_of(z, y, 1 - core)).astype(bf16)
        o1_copy(i).start()

    for_sibling(0)

    @pl.loop(0, nz)
    def _(i):
        for_sibling(i + 1)
        z, y = target(i, 1 - yy)
        value = project(rank_of(z, y, core))
        o1_copy(i).wait_recv()
        oy[i] = (value + ro1[i].astype(f32)).astype(bf16)
        o2_copy(i).start()

    def out_part(i):
        z, y = target(nz + i, 1 - yy)
        value = project(rank_of(z, y, core))
        o1_copy(nz + i).wait_recv()
        value = value + ro1[nz + i].astype(f32)
        o2_copy(i).wait_recv()
        return value + ro2[i].astype(f32)

    @pl.loop(0, nz - 1)
    def _(i):
        for_sibling(nz + i + 1)
        k = off(i + 1)
        oz[k] = out_part(i).astype(bf16)
        o3_copy(k).start()

    summed = out_part(nz - 1)
    for k in range(1, nz):
        o3_copy(k).wait_recv()
        summed = summed + ro3[k].astype(f32)
    hidden = (tok[...].astype(f32) + summed).astype(bf16)
    wide = hidden.astype(f32)
    hid_v[...] = hidden
    hid_copy = pltpu.make_async_copy(hid_v, out.at[0], s_out.at[0])
    hid_copy.start()
    square = jnp.sum(wide * wide, axis=1, keepdims=True)
    diagonal = (
        lax.broadcasted_iota(jnp.int32, (rows, HD), 0)
        == lax.broadcasted_iota(jnp.int32, (rows, HD), 1))
    ss[0] = jnp.sum(jnp.where(diagonal, square, 0.0), axis=0, keepdims=True)

    def ss_copy(k):
        return rcopy(ss.at[0], ss.at[k], ss_s.at[k], ss_r.at[k], lax.rem(me + k, n))

    @pl.loop(1, n)
    def _(k):
        ss_copy(k).start()

    total = ss[0]
    for k in range(1, n):
        ss_copy(k).wait_recv()
        total = total + ss[k]
    mean = jnp.sum(jnp.where(diagonal, total, 0.0), axis=1, keepdims=True) / (n * width)
    row_scale = lax.rsqrt(mean + epsilon)
    post = post_in[...].astype(f32)
    for i in range(width // HD):
        part = slice(i * HD, (i + 1) * HD)
        nrm_v[:, part] = (wide[:, part] * row_scale * post[i:i + 1]).astype(bf16)
    nrm_copy = pltpu.make_async_copy(nrm_v, out.at[1], s_out.at[1])
    nrm_copy.start()

    @pl.loop(1, nz)
    def _(k):
        tz(k).wait_send()
        qz(k).wait_send()
        a3_copy(k).wait_send()
        a3s_copy(k).wait_send()
        o3_copy(k).wait_send()

    @pl.loop(0, nz)
    def _(k):
        ty(k, tok).wait_send()
        qy(k, own_q).wait_send()
        a2_copy(k).wait_send()
        a2s_copy(k).wait_send()
        o2_copy(k).wait_send()

    @pl.loop(0, half)
    def _(k):
        tc(k, me, tok).wait_send()
        qc(k, me, own_q).wait_send()
        a1_copy(k).wait_send()
        a1s_copy(k).wait_send()
        o1_copy(k).wait_send()

    @pl.loop(1, half)
    def _(k):
        kv_copy(k).wait_send()

    @pl.loop(1, n)
    def _(k):
        ss_copy(k).wait_send()

    kv_pair.wait_send()
    kv_out.wait_send()
    hid_copy.wait()
    nrm_copy.wait()


def local(n, tokens, in_gain, w_query, w_key, w_value, w_out, cache_keys, cache_values, lengths,
          post_gain):
    rows, width = tokens.shape
    cols = w_query.shape[1]
    span = cache_keys.shape[1]
    kv_width = w_key.shape[1]
    heads_dev = cols // HD
    head_cols = heads_dev * rows
    nz, half = n // 4, n // 2
    vm = pl.BlockSpec(memory_space=pltpu.VMEM)
    hbm = pl.BlockSpec(memory_space=pl.ANY)
    V = pltpu.VMEM
    dma = lambda k: pltpu.SemaphoreType.DMA((k,))
    attn = lambda k: V((k, HD, head_cols), bf16)
    stat = lambda k: V((k, 2, head_cols), f32)
    block = lambda k: V((k, rows, width), bf16)
    scratch = [
        V((1, n * width), f32), V((rows, HD), f32), V((rows, HD), f32),
        V((rows, width), bf16), V((rows, width), bf16), dma(2),
        V((n, width, cols), bf16), V((width, kv_width), bf16), V((width, kv_width), bf16),
        V((n, cols, width), bf16), V(cache_keys.shape, bf16), V(cache_values.shape, bf16),
        block(n), V((n, rows, cols), bf16), V((rows, cols), f32), V((rows, HD), f32),
        V((rows * span, GROUP * rows), f32),
        V((2, KVH, rows, HD), bf16), V((KVH, rows, HD), bf16), V((KVH, rows, HD), bf16),
        V((half, rows, HD), bf16), V((2, rows, HD), f32),
        V((2, half, HD, head_cols), bf16), V((2, half, 2, head_cols), f32),
        attn(half), stat(half), attn(nz), stat(nz), attn(nz), stat(nz), attn(nz), stat(nz),
        attn(nz), stat(nz),
        block(half), block(half), block(nz), block(nz), block(nz), block(nz),
        V((n, 1, HD), f32),
        dma(4), dma(n), dma(n),
        dma(nz), dma(nz), dma(nz), dma(nz), dma(half), dma(half),
        dma(nz), dma(nz), dma(nz), dma(nz), dma(half), dma(half),
        dma(half), dma(half), dma(1), dma(1),
        dma(n), dma(n), dma(half), dma(half), dma(half), dma(half),
        dma(half), dma(half), dma(nz), dma(nz), dma(nz), dma(nz), dma(n), dma(n),
    ]
    both = pl.pallas_call(
        functools.partial(kernel, n, rows, width, cols, span),
        out_shape=jax.ShapeDtypeStruct((2, rows, width), bf16),
        in_specs=[vm, vm, vm, vm, hbm, hbm, hbm, hbm, hbm, hbm],
        out_specs=hbm,
        scratch_shapes=scratch,
        compiler_params=pltpu.CompilerParams(
            collective_id=0, has_side_effects=True, vmem_limit_bytes=67043328),
    )(
        tokens, in_gain.reshape(-1, HD), post_gain.reshape(-1, HD), lengths[None, :], w_query,
        w_key, w_value, w_out, cache_keys, cache_values,
    )
    return both[0], both[1]


def solution(mesh):
    placed = (
        P("replica", "tp"),
        P(),
        P(None, "tp"),
        P("tp", None),
        P("tp", None),
        P("tp", None),
        P("replica", "tp", None),
        P("replica", "tp", None),
        P("replica"),
        P("tp"),
    )
    return jax.shard_map(
        functools.partial(local, mesh.shape["tp"]),
        mesh=mesh,
        in_specs=placed,
        out_specs=(P("replica", "tp"), P("replica", "tp")),
        check_vma=False,
    )
```
